16 devices in a mesh: dp: 2 (over y, z), pp: 8 (over x, core).
Axes of the slice: x: 4, y: 2, z: 1, core: 2. Of those that a mesh axis runs over, the one named last changes fastest.
The devices are a block of a 4x4x8 slice.
Arguments:
- acts_in: bfloat16 [16, 8, 192, 768], P(None, 'dp'), parts along dimension 1
- cotangent: bfloat16 [16, 8, 192, 768], P(None, 'dp'), parts along dimension 1
- ln1_gain: bfloat16 [8, 768], P('pp')
- ln1_shift: bfloat16 [8, 768], P('pp')
- w_qkv: bfloat16 [8, 768, 2304], P('pp')
- b_qkv: bfloat16 [8, 2304], P('pp')
- w_proj: bfloat16 [8, 12, 64, 768], P('pp')
- b_proj: bfloat16 [8, 768], P('pp')
- ln2_gain: bfloat16 [8, 768], P('pp')
- ln2_shift: bfloat16 [8, 768], P('pp')
- w_up: bfloat16 [8, 768, 3072], P('pp')
- b_up: bfloat16 [8, 3072], P('pp')
- w_down: bfloat16 [8, 3072, 768], P('pp')
- b_down: bfloat16 [8, 768], P('pp')
Outputs:
- output 1: bfloat16 [16, 8, 192, 768], P(None, 'dp'), parts along dimension 1
- output 2: bfloat16 [16, 8, 192, 768], P(None, 'dp'), parts along dimension 1
- output 3: float32 [16, 768], P(('dp', 'pp')), parts along dimension 0
- output 4: float32 [16, 768], P(('dp', 'pp')), parts along dimension 0
- output 5: float32 [16, 768, 2304], P(('dp', 'pp')), parts along dimension 0
- output 6: float32 [16, 2304], P(('dp', 'pp')), parts along dimension 0
- output 7: float32 [16, 12, 64, 768], P(('dp', 'pp')), parts along dimension 0
- output 8: float32 [16, 768], P(('dp', 'pp')), parts along dimension 0
- output 9: float32 [16, 768], P(('dp', 'pp')), parts along dimension 0
- output 10: float32 [16, 768], P(('dp', 'pp')), parts along dimension 0
- output 11: float32 [16, 768, 3072], P(('dp', 'pp')), parts along dimension 0
- output 12: float32 [16, 3072], P(('dp', 'pp')), parts along dimension 0
- output 13: float32 [16, 3072, 768], P(('dp', 'pp')), parts along dimension 0
- output 14: float32 [16, 768], P(('dp', 'pp')), parts along dimension 0
There are 2 independent parts. The reference program is written for one: setup_inputs(seed, part) draws one part's arguments, and reference() takes and returns one part's arrays. A program takes and returns all parts, laid end to end along the dimension named above; an argument that names none is the same for every part.
All inputs are finite; a program needn't handle non-finite values.
Results may differ from the reference program's by a relative error of at most 0.02.
Values are sent between devices in bfloat16 or wider.
A program may use at most 768 MiB of HBM per device.

```python
import jax
import jax.numpy as jnp
from jax import lax

D = 768
HEADS = 12
LAYERS = 8
MICRO = 16
BATCH = 4
SEQ = 192
HEAD = D // HEADS
TOKENS = BATCH * SEQ
LN_EPS = 1e-5


def setup_inputs(seed: int = 0, part: int = 0) -> dict:
    part_key = jax.random.fold_in(jax.random.key(seed), part)
    key_x, key_ct = jax.random.split(part_key)
    key_list = jax.random.split(jax.random.key(seed + 1), 12)
    act_shape = (MICRO, BATCH, SEQ, D)

    def draw_normal(rng_key, arr_dims, scale_by):
        return jax.random.normal(rng_key, arr_dims, jnp.float32) * scale_by

    return {
        'acts_in': draw_normal(key_x, act_shape, 1.0).astype(jnp.bfloat16),
        'cotangent': draw_normal(key_ct, act_shape, 1.0).astype(jnp.bfloat16),
        'ln1_gain': (1.0 + draw_normal(key_list[0], (LAYERS, D), 0.2)).astype(jnp.bfloat16),
        'ln1_shift': draw_normal(key_list[1], (LAYERS, D), 0.3).astype(jnp.bfloat16),
        'w_qkv': draw_normal(key_list[2], (LAYERS, D, 3 * D), D ** -0.5).astype(jnp.bfloat16),
        'b_qkv': draw_normal(key_list[3], (LAYERS, 3 * D), 0.3).astype(jnp.bfloat16),
        'w_proj': draw_normal(key_list[4], (LAYERS, HEADS, HEAD, D), D ** -0.5).astype(jnp.bfloat16),
        'b_proj': draw_normal(key_list[5], (LAYERS, D), 0.3).astype(jnp.bfloat16),
        'ln2_gain': (1.0 + draw_normal(key_list[6], (LAYERS, D), 0.2)).astype(jnp.bfloat16),
        'ln2_shift': draw_normal(key_list[7], (LAYERS, D), 0.3).astype(jnp.bfloat16),
        'w_up': draw_normal(key_list[8], (LAYERS, D, 4 * D), D ** -0.5).astype(jnp.bfloat16),
        'b_up': draw_normal(key_list[9], (LAYERS, 4 * D), 0.3).astype(jnp.bfloat16),
        'w_down': draw_normal(key_list[10], (LAYERS, 4 * D, D), (4 * D) ** -0.5).astype(jnp.bfloat16),
        'b_down': draw_normal(key_list[11], (LAYERS, D), 0.3).astype(jnp.bfloat16),
    }


def layer_norm(x_wide, gain, shift):
    mean_val = jnp.mean(x_wide, axis=-1, keepdims=True)
    centered = x_wide - mean_val
    variance = jnp.mean(centered * centered, axis=-1, keepdims=True)
    return centered * lax.rsqrt(variance + LN_EPS) * gain + shift


def mat_mul(act_rows, weight):
    return jnp.dot(act_rows.astype(jnp.float32), weight, preferred_element_type=jnp.float32)


def layer_forward(weights, x_act):
    g_one, s_one, w_qkv, b_qkv, w_proj, b_proj, g_two, s_two, w_up, b_up, w_down, b_down = weights
    x_wide = x_act.astype(jnp.float32)
    h_one = layer_norm(x_wide, g_one, s_one).astype(jnp.bfloat16)
    qkv_act = (mat_mul(h_one, w_qkv) + b_qkv).astype(jnp.bfloat16)
    qkv_heads = qkv_act.astype(jnp.float32).reshape(BATCH, SEQ, 3, HEADS, HEAD)
    scores = jnp.einsum('bqhd,bkhd->bhqk', qkv_heads[:, :, 0], qkv_heads[:, :, 1]) * (HEAD ** -0.5)
    causal = jnp.arange(SEQ)[:, None] >= jnp.arange(SEQ)[None, :]
    attn_probs = jax.nn.softmax(jnp.where(causal, scores, -1e30), axis=-1).astype(jnp.bfloat16)
    attn_mix = jnp.einsum('bhqk,bkhd->bqhd', attn_probs.astype(jnp.float32), qkv_heads[:, :, 2]).astype(jnp.bfloat16)
    x_mid = (x_wide + mat_mul(attn_mix.reshape(TOKENS, D), w_proj.reshape(D, D)) + b_proj).astype(jnp.bfloat16)
    mid_wide = x_mid.astype(jnp.float32)
    h_two = layer_norm(mid_wide, g_two, s_two).astype(jnp.bfloat16)
    hidden = jax.nn.gelu(mat_mul(h_two, w_up) + b_up, approximate=True).astype(jnp.bfloat16)
    return (mid_wide + mat_mul(hidden, w_down) + b_down).astype(jnp.bfloat16)


def reference(acts_in, cotangent, ln1_gain, ln1_shift, w_qkv, b_qkv, w_proj, b_proj, ln2_gain, ln2_shift, w_up, b_up, w_down, b_down):
    weights = tuple(tensor.astype(jnp.float32) for tensor in (ln1_gain, ln1_shift, w_qkv, b_qkv, w_proj, b_proj, ln2_gain, ln2_shift, w_up, b_up, w_down, b_down))

    def stack_forward(stack_w, x_act):
        def layer_step(carry_act, layer_w):
            return layer_forward(layer_w, carry_act), None
        final_act, unused = lax.scan(layer_step, x_act, stack_w)
        return final_act

    def micro_step(grad_acc, mb_pair):
        x_mb, ct_mb = mb_pair
        y_rows, pull_back = jax.vjp(stack_forward, weights, x_mb.reshape(TOKENS, D))
        w_grads, x_grad = pull_back(ct_mb.reshape(TOKENS, D))
        new_acc = tuple(acc_old + new_grad for acc_old, new_grad in zip(grad_acc, w_grads))
        return new_acc, (y_rows.reshape(BATCH, SEQ, D), x_grad.reshape(BATCH, SEQ, D))

    zero_acc = tuple(jnp.zeros_like(tensor) for tensor in weights)
    grad_sums, (acts_out, grad_in) = lax.scan(micro_step, zero_acc, (acts_in, cotangent))
    return (acts_out, grad_in, grad_sums[0], grad_sums[1], grad_sums[2], grad_sums[3], grad_sums[4], grad_sums[5], grad_sums[6], grad_sums[7], grad_sums[8], grad_sums[9], grad_sums[10], grad_sums[11])
```

```python
import functools

import jax
import jax.numpy as jnp
from jax import lax
from jax.experimental import pallas as pl
from jax.experimental.pallas import tpu as pltpu
from jax.sharding import PartitionSpec as P

LN_EPS = 1e-5
PARAM_RANKS = (2, 2, 3, 2, 4, 2, 2, 2, 3, 2, 3, 2)
F32, BF16 = jnp.float32, jnp.bfloat16
PAIR = 128


def normalize(x_wide):
    mean_val = jnp.mean(x_wide, axis=-1, keepdims=True)
    centered = x_wide - mean_val
    variance = jnp.mean(centered * centered, axis=-1, keepdims=True)
    inv_std = lax.rsqrt(variance + LN_EPS)
    return centered * inv_std, inv_std


def normalize_back(grad_h, gain, x_hat, inv_std):
    grad_hat = grad_h * gain
    mean_grad = jnp.mean(grad_hat, axis=-1, keepdims=True)
    mean_dot = jnp.mean(grad_hat * x_hat, axis=-1, keepdims=True)
    return inv_std * (grad_hat - mean_grad - x_hat * mean_dot)


def gelu_tanh(pre_act):
    return jax.nn.gelu(pre_act, approximate=True)


def mat(lhs, rhs, lhs_dim=1, rhs_dim=0):
    return lax.dot_general(lhs, rhs, (((lhs_dim,), (rhs_dim,)), ((), ())), preferred_element_type=F32)


def head_probs(q_pair, k_pair, in_head, causal, scale):
    q_head = jnp.where(in_head, q_pair, jnp.zeros_like(q_pair))
    scores = jnp.where(causal, mat(q_head, k_pair, 1, 1) * scale, -1e30)
    exps = jnp.exp(scores - jnp.max(scores, axis=-1, keepdims=True))
    return (exps * (1.0 / jnp.sum(exps, axis=-1, keepdims=True))).astype(BF16)


def masks(n_seq, head_dim):
    lanes = lax.broadcasted_iota(jnp.int32, (n_seq, PAIR), 1)
    causal = lax.broadcasted_iota(jnp.int32, (n_seq, n_seq), 0) >= lax.broadcasted_iota(jnp.int32, (n_seq, n_seq), 1)
    return (lanes < head_dim, lanes >= head_dim), causal


def attn_fwd_kernel(head_dim, place, qkv_ref, o_old, o_ref):
    n_seq, width = o_ref.shape[2], o_ref.shape[3]
    in_heads, causal = masks(n_seq, head_dim)
    for col in range(0, width, PAIR):
        q_pair, k_pair, v_pair = (qkv_ref[0, 0, :, part * width + col:part * width + col + PAIR] for part in range(3))
        mixes = [mat(head_probs(q_pair, k_pair, in_head, causal, head_dim ** -0.5), v_pair) for in_head in in_heads]
        o_ref[0, 0, :, col:col + PAIR] = jnp.where(in_heads[0], mixes[0], mixes[1]).astype(BF16)


def attn_bwd_kernel(head_dim, place, qkv_ref, go_ref, g_old, g_ref):
    n_seq, width = go_ref.shape[1], go_ref.shape[2]
    in_heads, _ = masks(n_seq, head_dim)
    causal = lax.broadcasted_iota(jnp.int32, (n_seq, n_seq), 0) <= lax.broadcasted_iota(jnp.int32, (n_seq, n_seq), 1)
    scale = head_dim ** -0.5
    for col in range(0, width, PAIR):
        q_pair, k_pair, v_pair = (qkv_ref[0, 0, :, part * width + col:part * width + col + PAIR] for part in range(3))
        go_pair = go_ref[0, :, col:col + PAIR]
        grads = []
        for in_head in in_heads:
            q_head = jnp.where(in_head, q_pair, jnp.zeros_like(q_pair))
            go_head = jnp.where(in_head, go_pair, jnp.zeros_like(go_pair))
            scores = jnp.where(causal, mat(k_pair, q_head, 1, 1) * scale, -1e30)
            exps = jnp.exp(scores - jnp.max(scores, axis=0, keepdims=True))
            probs = (exps * (1.0 / jnp.sum(exps, axis=0, keepdims=True))).astype(BF16)
            grad_probs = mat(v_pair, go_head, 1, 1).astype(BF16).astype(F32)
            wide = probs.astype(F32)
            row_dot = jnp.sum(grad_probs * wide, axis=0, keepdims=True)
            grad_scores = (wide * (grad_probs - row_dot) * scale).astype(BF16)
            grads.append((mat(grad_scores, k_pair, 0, 0), mat(grad_scores, q_pair), mat(probs, go_pair)))
        for part in range(3):
            g_ref[0, 0, :, part * width + col:part * width + col + PAIR] = jnp.where(in_heads[0], grads[0][part], grads[1][part]).astype(BF16)


def attn_cost(n_rows, n_seq, width, dots):
    return pl.CostEstimate(flops=dots * 8 * n_rows * n_seq * n_seq * width, bytes_accessed=n_rows * n_seq * width * 14, transcendentals=0)


def attn_fwd(place, qkv_all, o_all, n_rows, head_dim):
    n_seq, width = o_all.shape[2:]
    spec = lambda cols: pl.BlockSpec((1, 1, n_seq, cols), lambda row, place: (place[0], place[1] + row, 0, 0))
    return pl.pallas_call(
        functools.partial(attn_fwd_kernel, head_dim),
        grid_spec=pltpu.PrefetchScalarGridSpec(
            num_scalar_prefetch=1, grid=(n_rows,),
            in_specs=[spec(3 * width), pl.BlockSpec(memory_space=pl.ANY)], out_specs=spec(width)),
        out_shape=jax.ShapeDtypeStruct(o_all.shape, BF16), input_output_aliases={2: 0},
        cost_estimate=attn_cost(n_rows, n_seq, width, 2), name="attn_fwd")(place, qkv_all, o_all)


def attn_bwd(place, qkv_all, grad_mix, g_all, head_dim):
    n_rows, n_seq, width = grad_mix.shape
    spec = lambda cols: pl.BlockSpec((1, 1, n_seq, cols), lambda row, place: (place[0], place[1] + row, 0, 0))
    return pl.pallas_call(
        functools.partial(attn_bwd_kernel, head_dim),
        grid_spec=pltpu.PrefetchScalarGridSpec(
            num_scalar_prefetch=1, grid=(n_rows,),
            in_specs=[spec(3 * width), pl.BlockSpec((1, n_seq, width), lambda row, place: (row, 0, 0)), pl.BlockSpec(memory_space=pl.ANY)],
            out_specs=spec(3 * width)),
        out_shape=jax.ShapeDtypeStruct(g_all.shape, BF16), input_output_aliases={3: 0},
        cost_estimate=attn_cost(n_rows, n_seq, width, 5), name="attn_bwd")(place, qkv_all, grad_mix, g_all)


def blank(*shapes):
    return pl.pallas_call(lambda *refs: None, out_shape=[jax.ShapeDtypeStruct(shape, BF16) for shape in shapes],
                          out_specs=[pl.BlockSpec(memory_space=pl.ANY)] * len(shapes), name="blank")()


def put(buf, value, mb, row):
    value = value.reshape((1, -1) + buf.shape[2:])
    return lax.dynamic_update_slice(buf, value, (mb, row, 0, 0))


def take(buf, mb, row, n_rows):
    return lax.dynamic_slice(buf, (mb, row, 0, 0), (1, n_rows) + buf.shape[2:]).reshape((-1,) + buf.shape[3:])


def half_forward(weights, x_act, bufs, mb, row, n_rows, head_dim):
    g_one, s_one, w_qkv, b_qkv, w_proj, b_proj, g_two, s_two, w_up, b_up, w_down, b_down = weights
    x_all, qkv_all, o_all, mid_all, y_all = bufs
    x_wide = x_act.astype(F32)
    h_one = (normalize(x_wide)[0] * g_one + s_one).astype(BF16)
    qkv_all = put(qkv_all, (mat(h_one, w_qkv) + b_qkv).astype(BF16), mb, row)
    o_all = attn_fwd(jnp.stack([mb, jnp.int32(row)]), qkv_all, o_all, n_rows, head_dim)
    x_mid = (x_wide + mat(take(o_all, mb, row, n_rows), w_proj) + b_proj).astype(BF16)
    mid_wide = x_mid.astype(F32)
    h_two = (normalize(mid_wide)[0] * g_two + s_two).astype(BF16)
    hidden = lax.optimization_barrier(gelu_tanh(mat(h_two, w_up) + b_up).astype(BF16))
    y_act = (mid_wide + mat(hidden, w_down) + b_down).astype(BF16)
    return y_act, (put(x_all, x_act, mb, row), qkv_all, o_all, put(mid_all, x_mid, mb, row), put(y_all, y_act, mb, row))


def half_backward(weights, saved, grad_y, bufs, mb, row, n_rows, head_dim):
    g_one, s_one, w_qkv, b_qkv, w_proj, b_proj, g_two, s_two, w_up, b_up, w_down, b_down = weights
    x_all, qkv_all, mid_all = saved
    gy_all, a_all, gpre_all, h2_all, gmid_all, gqkv_all, h1_all, dx_all = bufs
    grad_wide = grad_y.astype(F32)
    hat_two, inv_two = normalize(take(mid_all, mb, row, n_rows).astype(F32))
    h_two = (hat_two * g_two + s_two).astype(BF16)
    grad_hidden = mat(grad_y, w_down, 1, 1).astype(BF16)
    hidden, gelu_pull = jax.vjp(gelu_tanh, mat(h_two, w_up) + b_up)
    grad_pre = gelu_pull(grad_hidden.astype(F32))[0]
    grad_pre_bf = grad_pre.astype(BF16)
    grad_h_two = mat(grad_pre_bf, w_up, 1, 1).astype(BF16).astype(F32)
    grad_mid = (grad_wide + normalize_back(grad_h_two, g_two, hat_two, inv_two)).astype(BF16)
    mid_f32 = grad_mid.astype(F32)
    grad_mix = mat(grad_mid, w_proj, 1, 1).astype(BF16)
    n_seq = gqkv_all.shape[2]
    gqkv_all = attn_bwd(jnp.stack([mb, jnp.int32(row)]), qkv_all, grad_mix.reshape(n_rows, n_seq, -1), gqkv_all, head_dim)
    grad_qkv = take(gqkv_all, mb, row, n_rows)
    hat_one, inv_one = normalize(take(x_all, mb, row, n_rows).astype(F32))
    h_one = (hat_one * g_one + s_one).astype(BF16)
    grad_h_one = mat(grad_qkv, w_qkv, 1, 1).astype(BF16).astype(F32)
    grad_x = (mid_f32 + normalize_back(grad_h_one, g_one, hat_one, inv_one)).astype(BF16)
    sums = (jnp.sum(grad_h_one * hat_one, 0), jnp.sum(grad_h_one, 0),
            jnp.sum(grad_h_two * hat_two, 0), jnp.sum(grad_h_two, 0), jnp.sum(grad_pre, 0))
    values = (grad_y, hidden.astype(BF16), grad_pre_bf, h_two, grad_mid, None, h_one, grad_x)
    bufs = tuple(gqkv_all if value is None else put(buf, value, mb, row) for buf, value in zip(bufs, values))
    return grad_x, bufs, sums


def solution(mesh):
    n_stages = mesh.shape['pp']
    last_stage = n_stages - 1
    fwd_pairs = [(source, source + 1) for source in range(n_stages - 1)]
    bwd_pairs = [(source + 1, source) for source in range(n_stages - 1)]
    act_spec = P(None, 'dp', None, None)
    param_specs = tuple(P(*(('pp',) + (None,) * (rank_n - 1))) for rank_n in PARAM_RANKS)
    grad_specs = tuple(P(*((('dp', 'pp'),) + (None,) * (rank_n - 1))) for rank_n in PARAM_RANKS)

    def stage_body(acts_in, cotangent, *stacked_w):
        weights = tuple(tensor[0].astype(F32) if tensor.ndim == 2 else tensor[0] for tensor in stacked_w)
        head_dim = stacked_w[4].shape[2]
        weights = weights[:4] + (weights[4].reshape(-1, weights[4].shape[-1]),) + weights[5:]
        stage_idx = lax.axis_index('pp')
        n_micro, n_rows, n_seq, n_width = acts_in.shape
        n_hidden = stacked_w[8].shape[2]
        half = n_rows // 2
        n_steps = n_micro + n_stages - 1
        sized = lambda width: (n_micro, n_rows, n_seq, width)
        no_rows = jnp.zeros((half * n_seq, n_width), BF16)
        slabs = blank(*(sized(w) for w in (n_width, 3 * n_width, n_width, n_width, n_width)))

        def fwd_step(step_idx, loop_state):
            in_top, sent_low, bufs = loop_state
            in_low = lax.ppermute(sent_low, 'pp', fwd_pairs)
            mb = jnp.clip(step_idx - stage_idx, 0, n_micro - 1)
            first = jnp.minimum(step_idx, n_micro - 1)
            x_top = jnp.where(stage_idx == 0, take(acts_in, first, 0, half), in_top)
            y_top, bufs = half_forward(weights, x_top, bufs, mb, 0, half, head_dim)
            in_top = lax.ppermute(y_top, 'pp', fwd_pairs)
            x_low = jnp.where(stage_idx == 0, take(acts_in, first, half, half), in_low)
            y_low, bufs = half_forward(weights, x_low, bufs, mb, half, half, head_dim)
            return in_top, y_low, bufs

        _, _, saved = lax.fori_loop(0, n_steps, fwd_step, (no_rows, no_rows, tuple(slabs)))
        x_all, qkv_all, o_all, mid_all, y_all = saved
        slabs = blank(*(sized(w) for w in (n_width, n_hidden, n_hidden, n_width, n_width, 3 * n_width, n_width, n_width)))

        def bwd_step(step_idx, loop_state):
            in_top, sent_low, bufs, sums = loop_state
            in_low = lax.ppermute(sent_low, 'pp', bwd_pairs)
            offset = step_idx - (last_stage - stage_idx)
            is_valid = (offset >= 0) & (offset < n_micro)
            mb = jnp.clip(n_micro - 1 - offset, 0, n_micro - 1)
            first = jnp.clip(n_micro - 1 - step_idx, 0, n_micro - 1)
            saved_now = (x_all, qkv_all, mid_all)
            g_top = jnp.where(stage_idx == last_stage, take(cotangent, first, 0, half), in_top)
            gx_top, bufs, sums_top = half_backward(weights, saved_now, g_top, bufs, mb, 0, half, head_dim)
            in_top = lax.ppermute(gx_top, 'pp', bwd_pairs)
            g_low = jnp.where(stage_idx == last_stage, take(cotangent, first, half, half), in_low)
            gx_low, bufs, sums_low = half_backward(weights, saved_now, g_low, bufs, mb, half, half, head_dim)
            sums = tuple(old + jnp.where(is_valid, top + low, 0.0) for old, top, low in zip(sums, sums_top, sums_low))
            return in_top, gx_low, bufs, sums

        zero_sums = tuple(jnp.zeros((w,), F32) for w in (n_width, n_width, n_width, n_width, n_hidden))
        init = (no_rows, no_rows, tuple(slabs), zero_sums)
        acts_out = lax.psum(jnp.where(stage_idx == last_stage, y_all, jnp.zeros_like(y_all)), 'pp')
        _, _, bufs, sums = lax.fori_loop(0, n_steps, bwd_step, init)
        gy_all, a_all, gpre_all, h2_all, gmid_all, gqkv_all, h1_all, dx_all = bufs
        grad_in = lax.psum(jnp.where(stage_idx == 0, dx_all, jnp.zeros_like(dx_all)), 'pp')
        over_tokens = lambda lhs, rhs: mat(lhs.reshape(-1, lhs.shape[-1]), rhs.reshape(-1, rhs.shape[-1]), 0, 0)
        grad_w_qkv = over_tokens(h1_all, gqkv_all)
        grad_w_proj = over_tokens(o_all, gmid_all).reshape(stacked_w[4].shape[1:])
        grad_w_up = over_tokens(h2_all, gpre_all)
        grad_w_down = over_tokens(a_all, gy_all)
        all_rows = lambda buf: jnp.sum(buf, axis=(0, 1, 2), dtype=F32)
        grads = (sums[0], sums[1], grad_w_qkv, all_rows(gqkv_all), grad_w_proj, all_rows(gmid_all), sums[2], sums[3], grad_w_up, sums[4], grad_w_down, all_rows(gy_all))
        return (acts_out, grad_in) + tuple(acc_sum[None] for acc_sum in grads)

    return jax.shard_map(stage_body, mesh=mesh, in_specs=(act_spec, act_spec) + param_specs, out_specs=(act_spec, act_spec) + grad_specs, check_vma=False)
```
